32 devices in a mesh: gx: 4 (over z), gy: 8 (over y, x, core).
Axes of the slice: x: 2, y: 2, z: 4, core: 2. Of those that a mesh axis runs over, the one named last changes fastest.
Arguments:
- stored_vectors: bfloat16 [2, 16, 32, 4096], P(None, None, 'gx', 'gy'), may hold values from -4 to 4
- disorder: float32 [2, 32, 4096], P(None, 'gx', 'gy'), may hold values from -1.5 to 1.5
- vacancy: int32 [2, 32, 4096], P(None, 'gx', 'gy'), may hold values 0 or 1
- plan: int32 [32], replicated, may hold values from 0 to 31, as said below
Outputs:
- local_moments: float32 [4, 2, 32, 4096], P(None, None, 'gx', 'gy')
- trace_moments: float32 [4, 16], replicated
The draws below stay inside these ranges and needn't reach their ends.
Inputs may be any that keep to these rules, and one draw needn't show every extreme that they name: plan is a permutation of 0 to 31; stored block b is held by the device at gy index b // 4. The 4 lattice blocks of one device come from 4 different devices, and the 4 stored blocks of one device go to 4 different devices.
All inputs are finite; a program needn't handle non-finite values. No bound on the sum of `vacancy` on one device may be relied on, other than what follows from the above.
Results may differ from the reference program's by a relative error of at most 0.0003.
Values may be sent and summed in bfloat16 or wider, within the bound.
A program may use at most 64 MiB of HBM per device.

```python
import jax
import jax.numpy as jnp

BLOCK = 128
NB = 4
R = 16
TERMS = 4
LX = 32
LY = 4096
NBLK = 32


def draw_plan(key, part):
    devices = NBLK // NB
    key_tau, key_rho, key_offset, key_slot = jax.random.split(jax.random.fold_in(key, 7), 4)
    relabel = jax.random.permutation(key_tau, devices)
    order = jax.random.permutation(key_rho, devices)
    offsets = jax.random.permutation(key_offset, devices)[:NB]
    slots = jax.random.permutation(key_slot, NB)
    receiver = jnp.arange(devices)[:, None]
    within = jnp.arange(NB)[None, :]
    source = relabel[(order[receiver] + offsets[within]) % devices]
    return (source * NB + slots[within]).reshape(-1).astype(jnp.int32)


def place_ends(drawn, rng, low, high):
    extent = drawn.shape
    place = [jax.random.randint(jax.random.fold_in(rng, axis), (), 0, extent[axis]) for axis in range(len(extent))]
    drawn = drawn.at[tuple(place)].set(low)
    longest = extent.index(max(extent))
    place[longest] = (place[longest] + 1) % extent[longest]
    return drawn.at[tuple(place)].set(high)


def shard_levels(stream_key, shape, cuts, smallest, top_value):
    loudness, own = 1.0, jax.random.fold_in(stream_key, 6)
    for position, blocks in cuts:
        heights = jnp.exp(jax.random.uniform(jax.random.fold_in(own, position), (blocks,), jnp.float32, smallest / len(cuts), top_value / len(cuts)))
        loudness = loudness * jnp.repeat(heights, shape[position] // blocks).reshape([-1 if axis == position else 1 for axis in range(len(shape))])
    return loudness


def normal_values(own_key, extent, width, most, shards=(), kind=jnp.bfloat16):
    result = jax.random.normal(own_key, extent, jnp.float32) * width
    if len(shards) > 0:
        result = shard_levels(own_key, extent, shards, -0.22, 0.18) * result
    return jnp.clip(result, min=-most, max=most).astype(kind)


def setup_inputs(seed: int = 0) -> dict:
    key_list = jax.random.split(jax.random.key(seed), 5)
    stored_vectors = normal_values(key_list[0], (2, R, LX, LY), 1.0, 4.0, ((2, 4), (3, 8)))
    disorder = jnp.clip(jax.random.uniform(key_list[1], (2, LX, LY), jnp.float32, -1.5, 1.5) * shard_levels(key_list[1], (2, LX, LY), ((1, 4), (2, 8)), -0.4, 0.0), -1.5, 1.5)
    vacancy = place_ends((jax.random.randint(key_list[2], (2, LX, LY), 0, 10) < 9).astype(jnp.int32), jax.random.fold_in(key_list[2], 1), 0, 1)
    plan = draw_plan(jax.random.fold_in(key_list[4], 71), 0)
    return {"stored_vectors": stored_vectors, "disorder": disorder, "vacancy": vacancy, "plan": plan}


HOP_NEAR = 1.0
HOP_NEXT = 0.3
TWIST_COS = 0.4535961214255773
TWIST_SIN = 0.8912073600614354
SPREAD = 6.5
NEAR_A = ((0, 0), (-1, 0), (0, -1))
NEAR_B = ((0, 0), (1, 0), (0, 1))
SECOND = ((1, 0), (-1, 1), (0, -1))


def collect_sum(fetch, field, shifts):
    total = fetch(field, shifts[0])
    for shift in shifts[1:]:
        total = total + fetch(field, shift)
    return total


def hamilton(fetch, real, imag, onsite, keep):
    backs = tuple((-a, -b) for a, b in SECOND)
    out_real = []
    out_imag = []
    for sublat, chiral, bonds in ((0, 1.0, NEAR_A), (1, -1.0, NEAR_B)):
        other = 1 - sublat
        near_real = collect_sum(fetch, real[other], bonds)
        forward_real = collect_sum(fetch, real[sublat], SECOND)
        backward_real = collect_sum(fetch, real[sublat], backs)
        centre_real = fetch(real[sublat], (0, 0))
        mixed_real = TWIST_COS * (forward_real + backward_real)
        mixed_imag = chiral * TWIST_SIN * (forward_real - backward_real)
        level = onsite[sublat][None]
        if imag is None:
            result_imag = HOP_NEXT * mixed_imag
        else:
            near_imag = collect_sum(fetch, imag[other], bonds)
            forward_imag = collect_sum(fetch, imag[sublat], SECOND)
            backward_imag = collect_sum(fetch, imag[sublat], backs)
            centre_imag = fetch(imag[sublat], (0, 0))
            mixed_real = mixed_real - chiral * TWIST_SIN * (forward_imag - backward_imag)
            mixed_imag = mixed_imag + TWIST_COS * (forward_imag + backward_imag)
            result_imag = level * centre_imag - HOP_NEAR * near_imag + HOP_NEXT * mixed_imag
        result_real = level * centre_real - HOP_NEAR * near_real + HOP_NEXT * mixed_real
        factor = keep[sublat][None] / SPREAD
        out_real.append(result_real * factor)
        out_imag.append(result_imag * factor)
    return jnp.stack(out_real), jnp.stack(out_imag)


def rolled(field, shift):
    return jnp.roll(field, (-shift[0], -shift[1]), axis=(1, 2))


def reference(stored_vectors, disorder, vacancy, plan):
    blocks = stored_vectors.reshape(2, R, LX, NBLK, BLOCK)
    lattice = jnp.take(blocks, plan.astype(jnp.int32), axis=3).reshape(2, R, LX, LY)
    keep = vacancy.astype(jnp.float32)
    start = lattice.astype(jnp.float32) * keep[:, None]
    locals_list = []
    traces = []
    previous_real, previous_imag = start, None
    current_real, current_imag = hamilton(rolled, start, None, disorder, keep)
    locals_list.append(jnp.sum(start * current_real, axis=1) / R)
    traces.append(jnp.sum(start * current_real, axis=(0, 2, 3)) / (2 * LX * LY))
    for term in range(1, TERMS):
        image_real, image_imag = hamilton(rolled, current_real, current_imag, disorder, keep)
        next_real = 2.0 * image_real - previous_real
        if previous_imag is None:
            next_imag = 2.0 * image_imag
        else:
            next_imag = 2.0 * image_imag - previous_imag
        previous_real, previous_imag = current_real, current_imag
        current_real, current_imag = next_real, next_imag
        locals_list.append(jnp.sum(start * current_real, axis=1) / R)
        traces.append(jnp.sum(start * current_real, axis=(0, 2, 3)) / (2 * LX * LY))
    return jnp.stack(locals_list), jnp.stack(traces)
```

```python
import functools

import jax
import jax.numpy as jnp
from jax import lax
from jax.experimental import pallas as pl
from jax.experimental.pallas import tpu as pltpu
from jax.sharding import PartitionSpec as P

BLOCK = 128
TERMS = 4
HOP_NEXT = 0.3
TWIST_COS = 0.4535961214255773
TWIST_SIN = 0.8912073600614354
SPREAD = 6.5
HALO = TERMS
MESH = pl.DeviceIdType.MESH
F32 = jnp.float32

WAYS = tuple((a, b) for a in (-1, 0, 1) for b in (-1, 0, 1) if (a, b) != (0, 0))


def rows_from(a, wide):
    if a == 0:
        return slice(HALO, HALO + wide)
    return slice(0, HALO) if a == 1 else slice(HALO + wide, 2 * HALO + wide)


def rows_to(a, wide):
    if a == 0:
        return slice(0, wide)
    return slice(wide - HALO, wide) if a == 1 else slice(0, HALO)


def exchange(
    nx, ny,
    plan_ref, stored_ref, disorder_ref, vacancy_ref,
    lattice_ref, level_ref, keep_ref,
    turned, send, recv, grid, side, level_x, level_y, vac_x, vac_y,
    a2a_send, a2a_recv, halo_send, halo_recv, site_send, site_recv,
):
    gx, gy = lax.axis_index("gx"), lax.axis_index("gy")
    wide, long = disorder_ref.shape[1], disorder_ref.shape[2]
    blocks = long // BLOCK

    def at(a, b):
        return (lax.rem(gx + a + nx, nx), lax.rem(gy + b + ny, ny))

    def copy(source, target, out_sem, in_sem, device):
        return pltpu.make_async_remote_copy(
            src_ref=source, dst_ref=target, send_sem=out_sem, recv_sem=in_sem,
            device_id=device, device_id_type=MESH,
        )

    barrier = pltpu.get_barrier_semaphore()
    greeted = [at(0, i) for i in range(1, ny)] + [at(a, b) for a, b in WAYS if a != 0]
    for device in greeted:
        pl.semaphore_signal(barrier, inc=1, device_id=device, device_id_type=MESH)

    for k in range(blocks):
        for s in range(2):
            piece = stored_ref[s, :, :, k * BLOCK : (k + 1) * BLOCK].astype(F32)
            turned[k, s] = jnp.transpose(piece, (1, 0, 2)).astype(jnp.bfloat16)

    def fill(target, place):
        block = turned[0]
        for k in range(1, blocks):
            wanted = plan_ref[target * blocks] == gy * blocks + k
            for j in range(1, blocks):
                wanted = wanted | (plan_ref[target * blocks + j] == gy * blocks + k)
            block = jnp.where(wanted, turned[k], block)
        place[...] = block

    order = list(range(1, ny))
    for i in order:
        fill(lax.rem(gy + i, ny), send.at[i])
    pl.semaphore_wait(barrier, len(greeted))
    moves = []
    for i in order:
        move = copy(send.at[i], recv.at[gy], a2a_send.at[i], a2a_recv.at[i], at(0, i))
        move.start()
        moves.append(move)
    sites = []
    for w, (a, b) in enumerate(WAYS):
        lanes = slice(0, long) if b == 0 else (
            slice(long - BLOCK, long) if b == 1 else slice(0, BLOCK))
        for t, (own, by_x, by_y) in enumerate(
            ((disorder_ref, level_x, level_y), (vacancy_ref, vac_x, vac_y))
        ):
            target = by_x.at[w] if b == 0 else by_y.at[w]
            move = copy(own.at[:, :, lanes], target, site_send.at[w, t], site_recv.at[w, t],
                        at(a, b))
            move.start()
            sites.append(move)
    fill(gy, recv.at[gy])

    for move in sites:
        move.wait()
    low = lax.broadcasted_iota(jnp.int32, (2, wide, BLOCK), 2) < BLOCK // 2
    for own, by_x, by_y, out in (
        (disorder_ref, level_x, level_y, level_ref),
        (vacancy_ref, vac_x, vac_y, keep_ref),
    ):
        for a in (-1, 0, 1):
            middle = own[...] if a == 0 else by_x[WAYS.index((a, 0))]
            edge = jnp.where(low, by_y[WAYS.index((a, -1))], by_y[WAYS.index((a, 1))])
            kept = rows_to(a, wide)
            out[:, rows_from(a, wide), 0:long] = middle[:, kept].astype(F32)
            out[:, rows_from(a, wide), long:] = edge[:, kept].astype(F32)

    for move in moves:
        move.wait()
    for k in range(blocks):
        stored = plan_ref[gy * blocks + k]
        block = recv[0]
        for p in range(1, ny):
            block = jnp.where(stored >= p * blocks, recv[p], block)
        grid[:, HALO : HALO + wide, :, k * BLOCK : (k + 1) * BLOCK] = block
    halos = []
    for w, (a, b) in enumerate(WAYS):
        own = rows_to(a, wide)
        rows = slice(own.start + HALO, own.stop + HALO)
        if b == 0:
            source, target = grid.at[:, rows, :, 0:long], grid.at[:, rows_from(a, wide), :, 0:long]
        else:
            lanes = slice(long - BLOCK, long) if b == 1 else slice(0, BLOCK)
            source = grid.at[:, rows, :, lanes]
            target = side.at[0 if b == -1 else 1, :, rows_from(a, wide)]
        move = copy(source, target, halo_send.at[w], halo_recv.at[w], at(a, b))
        move.start()
        halos.append(move)
    for move in halos:
        move.wait()
    low = lax.broadcasted_iota(jnp.int32, grid.shape[:3] + (BLOCK,), 3) < BLOCK // 2
    lattice_ref[:, :, :, 0:long] = grid[...]
    lattice_ref[:, :, :, long:] = jnp.where(
        low, side[0].astype(F32), side[1].astype(F32)).astype(jnp.bfloat16)


def chebyshev(
    lattice_ref, level_ref, keep_ref, moments_ref, trace_ref,
    real0, imag0, real1, imag1, onsite, factor, traces,
):
    tall, vectors, extent = lattice_ref.shape[1:]
    wide, long = moments_ref.shape[2], moments_ref.shape[3]
    halves = vectors // 8
    cos, sin = HOP_NEXT * TWIST_COS, HOP_NEXT * TWIST_SIN

    factor[...] = keep_ref[...] * (1.0 / SPREAD)
    onsite[...] = level_ref[...] * factor[...]
    traces[...] = jnp.zeros_like(traces)

    @pl.loop(0, tall)
    def _(x):
        for s in range(2):
            mask = keep_ref[s, pl.ds(x, 1), :]
            real0[s, x] = lattice_ref[s, x].astype(F32) * mask

    def back(value):
        return pltpu.roll(value, 1, axis=1)

    def ahead(value):
        return pltpu.roll(value, extent - 1, axis=1)

    def bond(r, i, first, second, chiral, want_imag):
        turn = chiral * sin
        out_real = cos * (r[first] + r[second])
        if i is not None:
            out_real = out_real - turn * (i[first] - i[second])
        out_imag = None
        if want_imag:
            out_imag = turn * (r[first] - r[second])
            if i is not None:
                out_imag = out_imag + cos * (i[first] + i[second])
        return out_real, out_imag

    for n in range(1, TERMS + 1):
        cur_r, cur_i = (real0, imag0) if n % 2 else (real1, imag1)
        new_r, new_i = (real1, imag1) if n % 2 else (real0, imag0)
        complex_in, want_imag, keep_new = n > 1, n < TERMS, n < TERMS

        def row(x, half, measured):
            r8 = pl.ds(half * 8, 8)
            reals = [[cur_r[s, x + d, r8, :] for d in (-1, 0, 1)] for s in range(2)]
            imags = [None, None]
            if complex_in:
                imags = [[cur_i[s, x + d, r8, :] for d in (-1, 0, 1)] for s in range(2)]
            for s, chiral in ((0, 1.0), (1, -1.0)):
                r, i = reals[s], imags[s]
                other_r, other_i = reals[1 - s], imags[1 - s]
                here = bond(r, i, 2, 0, chiral, want_imag)
                behind = bond(r, i, 1, 2, chiral, want_imag)
                front = bond(r, i, 0, 1, chiral, want_imag)
                level = onsite[s, pl.ds(x, 1), :]
                scale = factor[s, pl.ds(x, 1), :]
                if n > 1:
                    level, scale = 2.0 * level, 2.0 * scale
                away = 0 if s == 0 else 2
                for part in range(2 if want_imag else 1):
                    own, other = (r, other_r) if part == 0 else (i, other_i)
                    hop, prior, later = here[part], behind[part], front[part]
                    if other is not None:
                        hop = hop - (other[1] + other[away])
                        if s == 0:
                            prior = prior - other[1]
                        else:
                            later = later - other[1]
                    result = (hop + (back(prior) + ahead(later))) * scale
                    if own is not None:
                        result = result + level * own[1]
                    store = new_r if part == 0 else new_i
                    if n == 2 and part == 0 or n > 2:
                        result = result - store[s, x, r8, :]
                    if keep_new:
                        store[s, x, r8, :] = result
                    if part == 0 and measured is not None:
                        start = lattice_ref[s, x].astype(F32)[half * 8 : half * 8 + 8]
                        start = start * keep_ref[s, pl.ds(x, 1), :]
                        measured(s, half, start[:, :long] * result[:, :long])

        def plain(x, carry):
            for half in range(halves):
                row(x, half, None)
            return carry

        def middle(x, carry):
            sums = [None, None]

            def measured(s, half, product):
                sums[s] = product if sums[s] is None else sums[s] + product
                total = traces[n - 1, half * 8 : half * 8 + 8, :]
                for k in range(long // BLOCK):
                    total = total + product[:, k * BLOCK : (k + 1) * BLOCK]
                traces[n - 1, half * 8 : half * 8 + 8, :] = total

            for half in range(halves):
                row(x, half, measured)
            for s in range(2):
                moments_ref[n - 1, s, pl.ds(x - HALO, 1), :] = (
                    jnp.sum(sums[s], axis=0, keepdims=True) * (1.0 / vectors))
            return carry

        if n < TERMS:
            lax.fori_loop(n, HALO, plain, 0)
        lax.fori_loop(HALO, HALO + wide, middle, 0)
        if n < TERMS:
            lax.fori_loop(HALO + wide, tall - n, plain, 0)

    lane = lax.broadcasted_iota(jnp.int32, (vectors, BLOCK), 1)
    gathered = jnp.zeros((vectors, BLOCK), F32)
    for n in range(TERMS):
        gathered = jnp.where(lane == n, jnp.sum(traces[n], axis=1, keepdims=True), gathered)
    trace_ref[...] = gathered


def local(nx, ny, stored_vectors, disorder, vacancy, plan):
    vectors, wide, long = stored_vectors.shape[1:]
    tall, extent = wide + 2 * HALO, long + BLOCK
    vmem = pl.BlockSpec(memory_space=pltpu.VMEM)
    bf16, i32 = jnp.bfloat16, jnp.int32
    dma = pltpu.SemaphoreType.DMA
    ways = len(WAYS)
    lattice, level, keep = pl.pallas_call(
        functools.partial(exchange, nx, ny),
        out_shape=(
            jax.ShapeDtypeStruct((2, tall, vectors, extent), bf16),
            jax.ShapeDtypeStruct((2, tall, extent), F32),
            jax.ShapeDtypeStruct((2, tall, extent), F32),
        ),
        in_specs=[pl.BlockSpec(memory_space=pltpu.SMEM), vmem, vmem, vmem],
        out_specs=(vmem,) * 3,
        scratch_shapes=[
            pltpu.VMEM((long // BLOCK, 2, wide, vectors, BLOCK), bf16),
            pltpu.VMEM((ny, 2, wide, vectors, BLOCK), bf16),
            pltpu.VMEM((ny, 2, wide, vectors, BLOCK), bf16),
            pltpu.VMEM((2, tall, vectors, long), bf16),
            pltpu.VMEM((2, 2, tall, vectors, BLOCK), bf16),
            pltpu.VMEM((ways, 2, wide, long), F32),
            pltpu.VMEM((ways, 2, wide, BLOCK), F32),
            pltpu.VMEM((ways, 2, wide, long), i32),
            pltpu.VMEM((ways, 2, wide, BLOCK), i32),
            dma((ny,)), dma((ny,)), dma((ways,)), dma((ways,)), dma((ways, 2)), dma((ways, 2)),
        ],
        compiler_params=pltpu.CompilerParams(collective_id=0, has_side_effects=True),
        name="exchange",
    )(plan, stored_vectors, disorder, vacancy)
    moments, trace = pl.pallas_call(
        chebyshev,
        out_shape=(
            jax.ShapeDtypeStruct((TERMS, 2, wide, long), F32),
            jax.ShapeDtypeStruct((vectors, BLOCK), F32),
        ),
        in_specs=[vmem] * 3,
        out_specs=(vmem,) * 2,
        scratch_shapes=[pltpu.VMEM((2, tall, vectors, extent), F32)] * 4
        + [pltpu.VMEM((2, tall, extent), F32)] * 2
        + [pltpu.VMEM((TERMS, vectors, BLOCK), F32)],
        name="chebyshev",
    )(lattice, level, keep)
    summed = lax.psum(trace[:, :TERMS].T, ("gx", "gy"))
    return moments, summed / (2 * wide * nx * long * ny)


def solution(mesh):
    placed = (P(None, None, "gx", "gy"), P(None, "gx", "gy"), P(None, "gx", "gy"), P())
    return jax.shard_map(
        functools.partial(local, mesh.shape["gx"], mesh.shape["gy"]),
        mesh=mesh,
        in_specs=placed,
        out_specs=(P(None, None, "gx", "gy"), P()),
        check_vma=False,
    )
```

```python
import functools

import jax
import jax.numpy as jnp
from jax import lax
from jax.experimental import pallas as pl
from jax.experimental.pallas import tpu as pltpu
from jax.sharding import PartitionSpec as P

BLOCK = 128
TERMS = 4
HOP_NEXT = 0.3
TWIST_COS = 0.4535961214255773
TWIST_SIN = 0.8912073600614354
SPREAD = 6.5
HALO = TERMS
MESH = pl.DeviceIdType.MESH
F32 = jnp.float32

WAYS = tuple((a, b) for a in (-1, 0, 1) for b in (-1, 0, 1) if (a, b) != (0, 0))


def rows_from(a, wide):
    if a == 0:
        return slice(HALO, HALO + wide)
    return slice(0, HALO) if a == 1 else slice(HALO + wide, 2 * HALO + wide)


def rows_to(a, wide):
    if a == 0:
        return slice(0, wide)
    return slice(wide - HALO, wide) if a == 1 else slice(0, HALO)


def program(
    nx, ny,
    plan_ref, stored_ref, disorder_ref, vacancy_ref,
    moments_ref, trace_ref,
    turned, send, recv, lattice, side, level_x, level_y, vac_x, vac_y, keep_ref, onsite, factor,
    real0, imag0, real1, imag1, traces, part, parts_y, parts_x,
    a2a_send, a2a_recv, halo_send, halo_recv, site_send, site_recv, sum_send, sum_recv,
):
    gx, gy = lax.axis_index("gx"), lax.axis_index("gy")
    wide, long = disorder_ref.shape[1], disorder_ref.shape[2]
    tall, vectors, extent = lattice.shape[1:]
    blocks = long // BLOCK
    halves = vectors // 8
    cos, sin = HOP_NEXT * TWIST_COS, HOP_NEXT * TWIST_SIN

    def at(a, b):
        return (lax.rem(gx + a + nx, nx), lax.rem(gy + b + ny, ny))

    def copy(source, target, out_sem, in_sem, device):
        return pltpu.make_async_remote_copy(
            src_ref=source, dst_ref=target, send_sem=out_sem, recv_sem=in_sem,
            device_id=device, device_id_type=MESH,
        )

    barrier = pltpu.get_barrier_semaphore()
    greeted = [at(0, i) for i in range(1, ny)] + [at(i, 0) for i in range(1, nx)]
    greeted += [at(a, b) for a, b in WAYS if a != 0 and b != 0]
    for device in greeted:
        pl.semaphore_signal(barrier, inc=1, device_id=device, device_id_type=MESH)

    for k in range(blocks):
        for s in range(2):
            piece = stored_ref[s, :, :, k * BLOCK : (k + 1) * BLOCK].astype(F32)
            turned[k, s] = jnp.transpose(piece, (1, 0, 2)).astype(jnp.bfloat16)

    def fill(target, place):
        block = turned[0]
        for k in range(1, blocks):
            wanted = plan_ref[target * blocks] == gy * blocks + k
            for j in range(1, blocks):
                wanted = wanted | (plan_ref[target * blocks + j] == gy * blocks + k)
            block = jnp.where(wanted, turned[k], block)
        place[...] = block

    for i in range(1, ny):
        fill(lax.rem(gy + i, ny), send.at[i])
    pl.semaphore_wait(barrier, len(greeted))
    moves = []
    for i in range(1, ny):
        move = copy(send.at[i], recv.at[gy], a2a_send.at[i], a2a_recv.at[i], at(0, i))
        move.start()
        moves.append(move)
    sites = []
    for w, (a, b) in enumerate(WAYS):
        lanes = slice(0, long) if b == 0 else (
            slice(long - BLOCK, long) if b == 1 else slice(0, BLOCK))
        for t, (own, by_x, by_y) in enumerate(
            ((disorder_ref, level_x, level_y), (vacancy_ref, vac_x, vac_y))
        ):
            target = by_x.at[w] if b == 0 else by_y.at[w]
            move = copy(own.at[:, :, lanes], target, site_send.at[w, t], site_recv.at[w, t],
                        at(a, b))
            move.start()
            sites.append(move)
    fill(gy, recv.at[gy])
    traces[...] = jnp.zeros_like(traces)

    for move in moves:
        move.wait()
    for k in range(blocks):
        stored = plan_ref[gy * blocks + k]
        block = recv[0]
        for p in range(1, ny):
            block = jnp.where(stored >= p * blocks, recv[p], block)
        lattice[:, HALO : HALO + wide, :, k * BLOCK : (k + 1) * BLOCK] = block
    halos = []
    for w, (a, b) in enumerate(WAYS):
        own = rows_to(a, wide)
        rows = slice(own.start + HALO, own.stop + HALO)
        if b == 0:
            source = lattice.at[:, rows, :, 0:long]
            target = lattice.at[:, rows_from(a, wide), :, 0:long]
        else:
            lanes = slice(long - BLOCK, long) if b == 1 else slice(0, BLOCK)
            source = lattice.at[:, rows, :, lanes]
            target = side.at[0 if b == -1 else 1, :, rows_from(a, wide)]
        move = copy(source, target, halo_send.at[w], halo_recv.at[w], at(a, b))
        move.start()
        halos.append(move)

    for move in sites:
        move.wait()
    low = lax.broadcasted_iota(jnp.int32, (2, wide, BLOCK), 2) < BLOCK // 2
    for own, by_x, by_y, out in (
        (disorder_ref, level_x, level_y, onsite),
        (vacancy_ref, vac_x, vac_y, keep_ref),
    ):
        for a in (-1, 0, 1):
            middle = own[...] if a == 0 else by_x[WAYS.index((a, 0))]
            edge = jnp.where(low, by_y[WAYS.index((a, -1))], by_y[WAYS.index((a, 1))])
            kept = rows_to(a, wide)
            out[:, rows_from(a, wide), 0:long] = middle[:, kept].astype(F32)
            out[:, rows_from(a, wide), long:] = edge[:, kept].astype(F32)
    factor[...] = keep_ref[...] * (1.0 / SPREAD)
    onsite[...] = onsite[...] * factor[...]

    for move in halos:
        move.wait()
    low = lax.broadcasted_iota(jnp.int32, (vectors, BLOCK), 1) < BLOCK // 2

    @pl.loop(0, tall)
    def _(x):
        for s in range(2):
            mask = keep_ref[s, pl.ds(x, 1), :]
            real0[s, x, :, 0:long] = lattice[s, x, :, 0:long].astype(F32) * mask[:, 0:long]
            edge = jnp.where(low, side[0, s, x].astype(F32), side[1, s, x].astype(F32))
            real0[s, x, :, long:] = edge * mask[:, long:]

    def back(value):
        return pltpu.roll(value, 1, axis=1)

    def ahead(value):
        return pltpu.roll(value, extent - 1, axis=1)

    def bond(r, i, first, second, chiral, want_imag):
        turn = chiral * sin
        out_real = cos * (r[first] + r[second])
        if i is not None:
            out_real = out_real - turn * (i[first] - i[second])
        out_imag = None
        if want_imag:
            out_imag = turn * (r[first] - r[second])
            if i is not None:
                out_imag = out_imag + cos * (i[first] + i[second])
        return out_real, out_imag

    for n in range(1, TERMS + 1):
        cur_r, cur_i = (real0, imag0) if n % 2 else (real1, imag1)
        new_r, new_i = (real1, imag1) if n % 2 else (real0, imag0)
        complex_in, want_imag, keep_new = n > 1, n < TERMS, n < TERMS

        def row(x, half, measured):
            r8 = pl.ds(half * 8, 8)
            reals = [[cur_r[s, x + d, r8, :] for d in (-1, 0, 1)] for s in range(2)]
            imags = [None, None]
            if complex_in:
                imags = [[cur_i[s, x + d, r8, :] for d in (-1, 0, 1)] for s in range(2)]
            for s, chiral in ((0, 1.0), (1, -1.0)):
                r, i = reals[s], imags[s]
                other_r, other_i = reals[1 - s], imags[1 - s]
                here = bond(r, i, 2, 0, chiral, want_imag)
                behind = bond(r, i, 1, 2, chiral, want_imag)
                front = bond(r, i, 0, 1, chiral, want_imag)
                level = onsite[s, pl.ds(x, 1), :]
                scale = factor[s, pl.ds(x, 1), :]
                if n > 1:
                    level, scale = 2.0 * level, 2.0 * scale
                away = 0 if s == 0 else 2
                for part in range(2 if want_imag else 1):
                    own, other = (r, other_r) if part == 0 else (i, other_i)
                    hop, prior, later = here[part], behind[part], front[part]
                    if other is not None:
                        hop = hop - (other[1] + other[away])
                        if s == 0:
                            prior = prior - other[1]
                        else:
                            later = later - other[1]
                    result = (hop + (back(prior) + ahead(later))) * scale
                    if own is not None:
                        result = result + level * own[1]
                    store = new_r if part == 0 else new_i
                    if n == 2 and part == 0 or n > 2:
                        result = result - store[s, x, r8, :]
                    if keep_new:
                        store[s, x, r8, :] = result
                    if part == 0 and measured is not None:
                        start = lattice[s, x, :, 0:long].astype(F32)[half * 8 : half * 8 + 8]
                        start = start * keep_ref[s, pl.ds(x, 1), 0:long]
                        measured(s, half, start * result[:, :long])

        def plain(x, carry):
            for half in range(halves):
                row(x, half, None)
            return carry

        def middle(x, carry):
            sums = [None, None]

            def measured(s, half, product):
                sums[s] = product if sums[s] is None else sums[s] + product
                total = traces[n - 1, half * 8 : half * 8 + 8, :]
                for k in range(long // BLOCK):
                    total = total + product[:, k * BLOCK : (k + 1) * BLOCK]
                traces[n - 1, half * 8 : half * 8 + 8, :] = total

            for half in range(halves):
                row(x, half, measured)
            for s in range(2):
                moments_ref[n - 1, s, pl.ds(x - HALO, 1), :] = (
                    jnp.sum(sums[s], axis=0, keepdims=True) * (1.0 / vectors))
            return carry

        if n < TERMS:
            lax.fori_loop(n, HALO, plain, 0)
        lax.fori_loop(HALO, HALO + wide, middle, 0)
        if n < TERMS:
            lax.fori_loop(HALO + wide, tall - n, plain, 0)

    slot = lax.broadcasted_iota(jnp.int32, (vectors, BLOCK), 0)
    lane = lax.broadcasted_iota(jnp.int32, (vectors, BLOCK), 1)
    part[...] = jnp.zeros_like(part)
    for n in range(TERMS):
        spread = jnp.where(slot == lane, jnp.sum(traces[n], axis=1, keepdims=True), 0.0)
        part[0, n : n + 1, :] = jnp.sum(spread, axis=0, keepdims=True)

    def gather(stage, count, me, slots, place):
        slots[me] = part[stage]
        sent = []
        for i in range(1, count):
            move = copy(part.at[stage], slots.at[me], sum_send.at[stage, i],
                        sum_recv.at[stage, i], place(i))
            move.start()
            sent.append(move)
        for move in sent:
            move.wait()
        total = slots[0]
        for p in range(1, count):
            total = total + slots[p]
        return total

    part[1] = gather(0, ny, gy, parts_y, lambda i: at(0, i))
    total = gather(1, nx, gx, parts_x, lambda i: at(i, 0))
    sites_total = 2 * wide * nx * long * ny
    trace_ref[...] = total[:TERMS, :vectors] * (1.0 / sites_total)


def local(nx, ny, stored_vectors, disorder, vacancy, plan):
    vectors, wide, long = stored_vectors.shape[1:]
    tall, extent = wide + 2 * HALO, long + BLOCK
    vmem = pl.BlockSpec(memory_space=pltpu.VMEM)
    bf16, i32 = jnp.bfloat16, jnp.int32
    dma = pltpu.SemaphoreType.DMA
    ways, most = len(WAYS), max(nx, ny)
    return pl.pallas_call(
        functools.partial(program, nx, ny),
        out_shape=(
            jax.ShapeDtypeStruct((TERMS, 2, wide, long), F32),
            jax.ShapeDtypeStruct((TERMS, vectors), F32),
        ),
        in_specs=[pl.BlockSpec(memory_space=pltpu.SMEM), vmem, vmem, vmem],
        out_specs=(vmem,) * 2,
        scratch_shapes=[
            pltpu.VMEM((long // BLOCK, 2, wide, vectors, BLOCK), bf16),
            pltpu.VMEM((ny, 2, wide, vectors, BLOCK), bf16),
            pltpu.VMEM((ny, 2, wide, vectors, BLOCK), bf16),
            pltpu.VMEM((2, tall, vectors, extent), bf16),
            pltpu.VMEM((2, 2, tall, vectors, BLOCK), bf16),
            pltpu.VMEM((ways, 2, wide, long), F32),
            pltpu.VMEM((ways, 2, wide, BLOCK), F32),
            pltpu.VMEM((ways, 2, wide, long), i32),
            pltpu.VMEM((ways, 2, wide, BLOCK), i32),
        ]
        + [pltpu.VMEM((2, tall, extent), F32)] * 3
        + [pltpu.VMEM((2, tall, vectors, extent), F32)] * 4
        + [
            pltpu.VMEM((TERMS, vectors, BLOCK), F32),
            pltpu.VMEM((2, 8, BLOCK), F32),
            pltpu.VMEM((ny, 8, BLOCK), F32),
            pltpu.VMEM((nx, 8, BLOCK), F32),
            dma((ny,)), dma((ny,)), dma((ways,)), dma((ways,)), dma((ways, 2)), dma((ways, 2)),
            dma((2, most)), dma((2, most)),
        ],
        compiler_params=pltpu.CompilerParams(collective_id=0, has_side_effects=True),
        name="chebyshev",
    )(plan, stored_vectors, disorder, vacancy)


def solution(mesh):
    placed = (P(None, None, "gx", "gy"), P(None, "gx", "gy"), P(None, "gx", "gy"), P())
    return jax.shard_map(
        functools.partial(local, mesh.shape["gx"], mesh.shape["gy"]),
        mesh=mesh,
        in_specs=placed,
        out_specs=(P(None, None, "gx", "gy"), P()),
        check_vma=False,
    )
```

```python
import functools

import jax
import jax.numpy as jnp
from jax import lax
from jax.experimental import pallas as pl
from jax.experimental.pallas import tpu as pltpu
from jax.sharding import PartitionSpec as P

BLOCK = 128
TERMS = 4
HOP_NEXT = 0.3
TWIST_COS = 0.4535961214255773
TWIST_SIN = 0.8912073600614354
SPREAD = 6.5
HALO = TERMS
MESH = pl.DeviceIdType.MESH
F32 = jnp.float32

WAYS = tuple((a, b) for a in (-1, 0, 1) for b in (-1, 0, 1) if (a, b) != (0, 0))


def rows_from(a, wide):
    if a == 0:
        return slice(HALO, HALO + wide)
    return slice(0, HALO) if a == 1 else slice(HALO + wide, 2 * HALO + wide)


def rows_to(a, wide):
    if a == 0:
        return slice(0, wide)
    return slice(wide - HALO, wide) if a == 1 else slice(0, HALO)


def program(
    nx, ny,
    plan_ref, stored_ref, disorder_ref, vacancy_ref,
    moments_ref, trace_ref,
    turned, send, recv, lattice, side, level_x, level_y, vac_x, vac_y, keep_ref, onsite, factor,
    real0, real1, real2, real3, imag1, imag2, imag3, traces, packs, part, parts_y, parts_x,
    a2a_send, a2a_recv, halo_send, halo_recv, site_send, site_recv, sum_send, sum_recv,
):
    gx, gy = lax.axis_index("gx"), lax.axis_index("gy")
    wide, long = disorder_ref.shape[1], disorder_ref.shape[2]
    tall, vectors = lattice.shape[1:3]
    extent = long + BLOCK
    blocks = long // BLOCK
    halves = vectors // 8
    cos, sin = HOP_NEXT * TWIST_COS, HOP_NEXT * TWIST_SIN

    def at(a, b):
        return (lax.rem(gx + a + nx, nx), lax.rem(gy + b + ny, ny))

    def copy(source, target, out_sem, in_sem, device):
        return pltpu.make_async_remote_copy(
            src_ref=source, dst_ref=target, send_sem=out_sem, recv_sem=in_sem,
            device_id=device, device_id_type=MESH,
        )

    barrier = pltpu.get_barrier_semaphore()
    greeted = [at(0, i) for i in range(1, ny)] + [at(i, 0) for i in range(1, nx)]
    greeted += [at(a, b) for a, b in WAYS if a != 0 and b != 0]
    for device in greeted:
        pl.semaphore_signal(barrier, inc=1, device_id=device, device_id_type=MESH)

    for k in range(blocks):
        for s in range(2):
            piece = stored_ref[s, :, :, k * BLOCK : (k + 1) * BLOCK].astype(F32)
            turned[k, s] = jnp.transpose(piece, (1, 0, 2)).astype(jnp.bfloat16)

    def fill(target, place):
        block = turned[0]
        for k in range(1, blocks):
            wanted = plan_ref[target * blocks] == gy * blocks + k
            for j in range(1, blocks):
                wanted = wanted | (plan_ref[target * blocks + j] == gy * blocks + k)
            block = jnp.where(wanted, turned[k], block)
        place[...] = block

    for i in range(1, ny):
        fill(lax.rem(gy + i, ny), send.at[i])
    pl.semaphore_wait(barrier, len(greeted))
    moves = []
    for i in range(1, ny):
        move = copy(send.at[i], recv.at[gy], a2a_send.at[i], a2a_recv.at[i], at(0, i))
        move.start()
        moves.append(move)
    sites = []
    for w, (a, b) in enumerate(WAYS):
        lanes = slice(0, long) if b == 0 else (
            slice(long - BLOCK, long) if b == 1 else slice(0, BLOCK))
        for t, (own, by_x, by_y) in enumerate(
            ((disorder_ref, level_x, level_y), (vacancy_ref, vac_x, vac_y))
        ):
            target = by_x.at[w] if b == 0 else by_y.at[w]
            move = copy(own.at[:, :, lanes], target, site_send.at[w, t], site_recv.at[w, t],
                        at(a, b))
            move.start()
            sites.append(move)
    fill(gy, recv.at[gy])
    traces[...] = jnp.zeros_like(traces)

    for move in moves:
        move.wait()
    for k in range(blocks):
        stored = plan_ref[gy * blocks + k]
        block = recv[0]
        for p in range(1, ny):
            block = jnp.where(stored >= p * blocks, recv[p], block)
        lattice[:, HALO : HALO + wide, :, k * BLOCK : (k + 1) * BLOCK] = block
    lane = lax.broadcasted_iota(jnp.int32, (vectors, BLOCK), 1)
    first = jnp.zeros((vectors, BLOCK), F32)
    last = jnp.zeros((vectors, BLOCK), F32)
    for s in range(2):
        for x in range(wide):
            shift = HALO * (s * wide + x)
            tile = lattice[s, HALO + x, :, 0:BLOCK].astype(F32)
            first = first + pltpu.roll(jnp.where(lane < HALO, tile, 0.0), shift, axis=1)
            tile = lattice[s, HALO + x, :, long - BLOCK : long].astype(F32)
            last = last + pltpu.roll(jnp.where(lane >= BLOCK - HALO, tile, 0.0), shift, axis=1)
    packs[0] = first.astype(jnp.bfloat16)
    packs[1] = last.astype(jnp.bfloat16)
    halos = {}
    for a, b in ((0, 1), (0, -1), (1, 0), (-1, 0), (1, 1), (1, -1), (-1, 1), (-1, -1)):
        w = WAYS.index((a, b))
        if b == 0:
            own = rows_to(a, wide)
            source = lattice.at[:, own.start + HALO : own.stop + HALO]
            target = lattice.at[:, rows_from(a, wide)]
        else:
            source, target = packs.at[0 if b == -1 else 1], side.at[w]
        halos[a, b] = copy(source, target, halo_send.at[w], halo_recv.at[w], at(a, b))
        halos[a, b].start()

    for move in sites:
        move.wait()
    low = lax.broadcasted_iota(jnp.int32, (2, wide, BLOCK), 2) < BLOCK // 2
    for own, by_x, by_y, out in (
        (disorder_ref, level_x, level_y, onsite),
        (vacancy_ref, vac_x, vac_y, keep_ref),
    ):
        for a in (-1, 0, 1):
            middle = own[...] if a == 0 else by_x[WAYS.index((a, 0))]
            edge = jnp.where(low, by_y[WAYS.index((a, -1))], by_y[WAYS.index((a, 1))])
            kept = rows_to(a, wide)
            out[:, rows_from(a, wide), 0:long] = middle[:, kept].astype(F32)
            out[:, rows_from(a, wide), long:] = edge[:, kept].astype(F32)
    factor[...] = keep_ref[...] * (1.0 / SPREAD)
    onsite[...] = onsite[...] * factor[...]

    def begin(a):
        rows, own = rows_from(a, wide), rows_to(a, wide)
        for s in range(2):
            for x in range(rows.start, rows.stop):
                mask = keep_ref[s, x : x + 1, :]
                shift = HALO * (s * wide + own.start + x - rows.start)
                shift = (BLOCK - shift) % BLOCK
                real0[s, x, :, 0:long] = lattice[s, x].astype(F32) * mask[:, 0:long]
                right = pltpu.roll(side[WAYS.index((a, -1))].astype(F32), shift, axis=1)
                left = pltpu.roll(side[WAYS.index((a, 1))].astype(F32), shift, axis=1)
                edge = jnp.where(lane < BLOCK // 2, right, left)
                real0[s, x, :, long:] = edge * mask[:, long:]

    def back(value):
        return pltpu.roll(value, 1, axis=1)

    def ahead(value):
        return pltpu.roll(value, extent - 1, axis=1)

    def bond(r, i, first, second, chiral, want_imag):
        turn = chiral * sin
        out_real = cos * (r[first] + r[second])
        if i is not None:
            out_real = out_real - turn * (i[first] - i[second])
        out_imag = None
        if want_imag:
            out_imag = turn * (r[first] - r[second])
            if i is not None:
                out_imag = out_imag + cos * (i[first] + i[second])
        return out_real, out_imag

    reals_of = (real0, real1, real2, real3)
    imags_of = (None, imag1, imag2, imag3)

    def term(n, count, where, measure):
        cur_r, cur_i = reals_of[n - 1], imags_of[n - 1]
        complex_in, want_imag, keep_new = n > 1, n < TERMS, n < TERMS

        def row(x, half, measured):
            r8 = pl.ds(half * 8, 8)
            reals = [[cur_r[s, x + d, r8, :] for d in (-1, 0, 1)] for s in range(2)]
            imags = [None, None]
            if complex_in:
                imags = [[cur_i[s, x + d, r8, :] for d in (-1, 0, 1)] for s in range(2)]
            for s, chiral in ((0, 1.0), (1, -1.0)):
                r, i = reals[s], imags[s]
                other_r, other_i = reals[1 - s], imags[1 - s]
                here = bond(r, i, 2, 0, chiral, want_imag)
                behind = bond(r, i, 1, 2, chiral, want_imag)
                front = bond(r, i, 0, 1, chiral, want_imag)
                level = onsite[s, pl.ds(x, 1), :]
                scale = factor[s, pl.ds(x, 1), :]
                if n > 1:
                    level, scale = 2.0 * level, 2.0 * scale
                away = 0 if s == 0 else 2
                results = []
                for part in range(2 if want_imag else 1):
                    own, other = (r, other_r) if part == 0 else (i, other_i)
                    hop, prior, later = here[part], behind[part], front[part]
                    if other is not None:
                        hop = hop - (other[1] + other[away])
                        if s == 0:
                            prior = prior - other[1]
                        else:
                            later = later - other[1]
                    result = (hop + (back(prior) + ahead(later))) * scale
                    if own is not None:
                        result = result + level * own[1]
                    fields = reals_of if part == 0 else imags_of
                    if n > 1 and fields[n - 2] is not None:
                        result = result - fields[n - 2][s, x, r8, :]
                    if keep_new:
                        fields[n][s, x, r8, :] = result
                    results.append(result[:, :long])
                if measured is not None:
                    measured(s, half, real0[s, x, r8, 0:long], results,
                             r[1][:, :long], None if i is None else i[1][:, :long])

        def plain(t, carry):
            x = where(t)
            for half in range(halves):
                row(x, half, None)
            return carry

        def middle(t, carry):
            x = where(t)
            sums = [None, None]

            def measured(s, half, start, results, now_r, now_i):
                product = start * results[0]
                sums[s] = product if sums[s] is None else sums[s] + product
                if n == 1:
                    extra = ((0, product), (4, start * start))
                elif n == 2:
                    extra = (
                        (1, product),
                        (2, now_r * results[0] + now_i * results[1]),
                        (3, results[0] * results[0] + results[1] * results[1]),
                    )
                else:
                    extra = ()
                for place, value in extra:
                    total = traces[place, half * 8 : half * 8 + 8, :]
                    for k in range(long // BLOCK):
                        total = total + value[:, k * BLOCK : (k + 1) * BLOCK]
                    traces[place, half * 8 : half * 8 + 8, :] = total

            for half in range(halves):
                row(x, half, measured)
            for s in range(2):
                moments_ref[n - 1, s, pl.ds(x - HALO, 1), :] = (
                    jnp.sum(sums[s], axis=0, keepdims=True) * (1.0 / vectors))
            return carry

        lax.fori_loop(0, count, middle if measure else plain, 0)

    def inside(n):
        term(n, wide - 2 * n, lambda t: HALO + n + t, True)

    def border(n):
        out = HALO - n
        term(n, 2 * out, lambda t: n + t + wide * (t // out), False)
        term(n, 2 * n, lambda t: HALO + t + (wide - 2 * n) * (t // n), True)

    for way in ((0, 1), (0, -1)):
        halos[way].wait()
    begin(0)
    for n in range(1, TERMS):
        inside(n)
    for way in WAYS:
        if way[0] != 0:
            halos[way].wait()
    begin(-1)
    begin(1)
    border(1)
    border(2)

    slot = lax.broadcasted_iota(jnp.int32, (vectors, BLOCK), 0)
    part[...] = jnp.zeros_like(part)
    for n in range(TERMS):
        value = traces[n]
        if n == 2:
            value = 2.0 * value - traces[0]
        if n == 3:
            value = 2.0 * value - traces[4]
        spread = jnp.where(slot == lane, jnp.sum(value, axis=1, keepdims=True), 0.0)
        part[0, n : n + 1, :] = jnp.sum(spread, axis=0, keepdims=True)

    def scatter(stage, count, me, slots, place):
        slots[me] = part[stage]
        sent = []
        for i in range(1, count):
            move = copy(part.at[stage], slots.at[me], sum_send.at[stage, i],
                        sum_recv.at[stage, i], place(i))
            move.start()
            sent.append(move)
        return sent

    def collect(sent, count, slots):
        for move in sent:
            move.wait()
        total = slots[0]
        for p in range(1, count):
            total = total + slots[p]
        return total

    sent = scatter(0, ny, gy, parts_y, lambda i: at(0, i))
    border(3)
    part[1] = collect(sent, ny, parts_y)
    sent = scatter(1, nx, gx, parts_x, lambda i: at(i, 0))
    term(TERMS, wide, lambda t: HALO + t, True)
    total = collect(sent, nx, parts_x)
    sites_total = 2 * wide * nx * long * ny
    trace_ref[...] = total[:TERMS, :vectors] * (1.0 / sites_total)


def local(nx, ny, stored_vectors, disorder, vacancy, plan):
    vectors, wide, long = stored_vectors.shape[1:]
    tall, extent = wide + 2 * HALO, long + BLOCK
    vmem = pl.BlockSpec(memory_space=pltpu.VMEM)
    bf16, i32 = jnp.bfloat16, jnp.int32
    dma = pltpu.SemaphoreType.DMA
    ways, most = len(WAYS), max(nx, ny)
    return pl.pallas_call(
        functools.partial(program, nx, ny),
        out_shape=(
            jax.ShapeDtypeStruct((TERMS, 2, wide, long), F32),
            jax.ShapeDtypeStruct((TERMS, vectors), F32),
        ),
        in_specs=[pl.BlockSpec(memory_space=pltpu.SMEM), vmem, vmem, vmem],
        out_specs=(vmem,) * 2,
        scratch_shapes=[
            pltpu.VMEM((long // BLOCK, 2, wide, vectors, BLOCK), bf16),
            pltpu.VMEM((ny, 2, wide, vectors, BLOCK), bf16),
            pltpu.VMEM((ny, 2, wide, vectors, BLOCK), bf16),
            pltpu.VMEM((2, tall, vectors, long), bf16),
            pltpu.VMEM((ways, vectors, BLOCK), bf16),
            pltpu.VMEM((ways, 2, wide, long), F32),
            pltpu.VMEM((ways, 2, wide, BLOCK), F32),
            pltpu.VMEM((ways, 2, wide, long), i32),
            pltpu.VMEM((ways, 2, wide, BLOCK), i32),
        ]
        + [pltpu.VMEM((2, tall, extent), F32)] * 3
        + [pltpu.VMEM((2, tall, vectors, extent), F32)] * 7
        + [
            pltpu.VMEM((TERMS + 1, vectors, BLOCK), F32),
            pltpu.VMEM((2, vectors, BLOCK), bf16),
            pltpu.VMEM((2, 8, BLOCK), F32),
            pltpu.VMEM((ny, 8, BLOCK), F32),
            pltpu.VMEM((nx, 8, BLOCK), F32),
            dma((ny,)), dma((ny,)), dma((ways,)), dma((ways,)), dma((ways, 2)), dma((ways, 2)),
            dma((2, most)), dma((2, most)),
        ],
        compiler_params=pltpu.CompilerParams(collective_id=0, has_side_effects=True),
        name="chebyshev",
    )(plan, stored_vectors, disorder, vacancy)


def solution(mesh):
    placed = (P(None, None, "gx", "gy"), P(None, "gx", "gy"), P(None, "gx", "gy"), P())
    return jax.shard_map(
        functools.partial(local, mesh.shape["gx"], mesh.shape["gy"]),
        mesh=mesh,
        in_specs=placed,
        out_specs=(P(None, None, "gx", "gy"), P()),
        check_vma=False,
    )
```
